32 devices in a mesh: freq: 8 (over y, x, core), feed: 4 (over z).
Axes of the slice: x: 2, y: 2, z: 4, core: 2. Of those that a mesh axis runs over, the one named last changes fastest.
Arguments:
- voltages: int32 [32, 2048, 2, 768], P(None, ('feed', 'freq')), may hold values from -127 to 127
- gains: float32 [2, 32, 2048], P(None, None, ('feed', 'freq')), may hold values from -0.06 to 0.06
Outputs:
- visibilities: float32 [32, 2, 2048, 2048], P('freq', None, 'feed')
The draws below stay inside these ranges and needn't reach their ends.
All inputs are finite; a program needn't handle non-finite values.
Results may differ from the reference program's by a relative error of at most 0.0031.
Values may be sent and summed in bfloat16 or wider, within the bound.
A program may use at most 192 MiB of HBM per device.

```python
import jax
import jax.numpy as jnp
from jax import lax

FEEDS = 2048
TIME = 768
CHAN = 32


def set_ends(array, rng, low, top_value):
    place = [jax.random.randint(jax.random.fold_in(rng, axis), (), 0, length) for axis, length in enumerate(array.shape)]
    longest = array.shape.index(max(array.shape))
    beside = place[:longest] + [(place[longest] + 1) % array.shape[longest]] + place[longest + 1:]
    return array.at[tuple(place)].set(low).at[tuple(beside)].set(top_value)


def block_scale(rng, dims, shards, least, top_value):
    loudness = 1.0
    for position, blocks in shards:
        draws = jax.random.uniform(jax.random.fold_in(jax.random.fold_in(rng, 6), position), (blocks,), jnp.float32, least / len(shards), top_value / len(shards))
        loudness = loudness * jnp.repeat(jnp.exp(draws), dims[position] // blocks).reshape((-1,) + (1,) * (len(dims) - 1 - position))
    return loudness


def gaussian(rng, dims, scale, limit, cuts=(), held_as=jnp.bfloat16):
    values = scale * jax.random.normal(rng, dims, jnp.float32)
    if cuts:
        values = values * block_scale(rng, dims, cuts, -0.22, 0.18)
    return jnp.clip(values, -limit, limit).astype(held_as)


def setup_inputs(seed: int = 0) -> dict:
    key_list = jax.random.split(jax.random.key(seed), 3)
    voltages = set_ends(jax.random.randint(key_list[0], (CHAN, FEEDS, 2, TIME), -127, 128), jax.random.fold_in(key_list[0], 1), -127, 127).astype(jnp.int32)
    gains = gaussian(key_list[1], (2, CHAN, FEEDS), 0.01, 0.06, ((2, 32),), jnp.float32)
    return {"voltages": voltages, "gains": gains}


def reference(voltages, gains):
    volt_real = voltages[:, :, 0, :].astype(jnp.float32)
    volt_imag = voltages[:, :, 1, :].astype(jnp.float32)
    gain_real = gains[0][:, :, None]
    gain_imag = gains[1][:, :, None]
    eq_real = gain_real * volt_real - gain_imag * volt_imag
    eq_imag = gain_real * volt_imag + gain_imag * volt_real
    equalized = jnp.stack([eq_real, eq_imag], axis=2).astype(jnp.bfloat16)

    def per_channel(block):
        columns = block.reshape(FEEDS, 2 * TIME)
        swapped = jnp.concatenate([block[:, 1, :], -block[:, 0, :]], axis=1)
        left_side = jnp.concatenate([columns, swapped], axis=0)
        result = jnp.dot(left_side, columns.T, preferred_element_type=jnp.float32)
        return result.reshape(2, FEEDS, FEEDS) * (1.0 / TIME)

    return lax.map(per_channel, equalized)
```

```python
import functools

import jax
import jax.numpy as jnp
from jax import lax
from jax.experimental import pallas as pl
from jax.experimental.pallas import tpu as pltpu
from jax.sharding import PartitionSpec as P

MESH = pl.DeviceIdType.MESH
ANY = pl.BlockSpec(memory_space=pl.ANY)
VMEM = pl.BlockSpec(memory_space=pltpu.VMEM)


def stack_rows(own_rows, samples):
    real_part = own_rows[..., :samples]
    imag_part = own_rows[..., samples:]
    swapped = jnp.concatenate([imag_part, -real_part], axis=-1)
    return jnp.stack([own_rows, swapped], axis=0)


def correlate(stacked, columns, samples):
    product = jnp.einsum("qrk,fk->qrf", stacked, columns, preferred_element_type=jnp.float32)
    return product * (1.0 / samples)


def ring_blocks(own, count):
    forward = [(source, (source + 1) % count) for source in range(count)]
    backward = [(source, (source - 1) % count) for source in range(count)]
    half = own.shape[0] // 2
    pieces = [(0, 0, own)]
    from_left = from_right = own
    for step in range(1, count):
        if 2 * step > count:
            break
        if 2 * step == count:
            pieces.append((-step, 0, lax.ppermute(from_left[:half], "feed", forward)))
            pieces.append((-step, half, lax.ppermute(from_right[half:], "feed", backward)))
        else:
            from_left = lax.ppermute(from_left, "feed", forward)
            from_right = lax.ppermute(from_right, "feed", backward)
            pieces.append((-step, 0, from_left))
            pieces.append((step, 0, from_right))
    return pieces


def ring_program(voltages, gains):
    channels, local_feeds, _, samples = voltages.shape
    freq_count = lax.axis_size("freq")
    feed_count = lax.axis_size("feed")
    position = lax.axis_index("feed")
    owned = channels // freq_count
    rows = local_feeds * freq_count
    volts = voltages.reshape(freq_count, owned, local_feeds, 2, samples)
    scale = gains.reshape(2, freq_count, owned, local_feeds)[..., None]
    visibilities = jnp.zeros((owned, 2, rows, rows * feed_count), jnp.float32)
    for channel in range(owned):
        volt_real = volts[:, channel, :, 0].astype(jnp.float32)
        volt_imag = volts[:, channel, :, 1].astype(jnp.float32)
        gain_real = scale[0, :, channel]
        gain_imag = scale[1, :, channel]
        eq_real = gain_real * volt_real - gain_imag * volt_imag
        eq_imag = gain_real * volt_imag + gain_imag * volt_real
        blocks = jnp.concatenate([eq_real, eq_imag], axis=-1).astype(jnp.bfloat16)
        arrived = lax.all_to_all(blocks, "freq", split_axis=0, concat_axis=0, tiled=True)
        own_rows = arrived.reshape(rows, 2 * samples)
        stacked = stack_rows(own_rows, samples)
        for offset, start, block in ring_blocks(own_rows, feed_count):
            owner = lax.rem(position + offset + feed_count, feed_count)
            visibilities = lax.dynamic_update_slice(
                visibilities,
                correlate(stacked, block, samples)[None],
                (channel, 0, 0, owner * rows + start),
            )
    return visibilities


def bit_flip(index, mask, count):
    total, bit = 0, 1
    while bit < count:
        total = total + ((index // bit + mask // bit) % 2) * bit
        bit *= 2
    return total


def line_kernel(
    geometry,
    volts,
    scale,
    out,
    held,
    staged,
    landed,
    wide,
    raw,
    sent,
    raw_sem,
    turn_send,
    turn_recv,
    out_send,
    out_recv,
    mid_send,
    mid_recv,
    vis_send,
    vis_recv,
    wide_sem,
):
    owned, freq_count, local_feeds, samples = geometry
    rows = freq_count * local_feeds
    pairs = freq_count // 2
    chunk = 2 * local_feeds
    stage_slots = staged.shape[0]
    raw_slots = raw.shape[0]
    blocks = owned * freq_count

    me = lax.axis_index("freq")
    plane = lax.axis_index("feed")
    my_pair = me // 2
    inner = (plane == 1) | (plane == 2)
    across = 3 - plane
    beside = jnp.where(plane < 2, 1 - plane, 5 - plane)

    barrier = pltpu.get_barrier_semaphore()
    for shift in range(1, freq_count):
        pl.semaphore_signal(
            barrier,
            inc=1,
            device_id=(bit_flip(me, shift, freq_count), plane),
            device_id_type=MESH,
        )
    pl.semaphore_signal(barrier, inc=1, device_id=(me, beside), device_id_type=MESH)

    @pl.when(inner)
    def _():
        pl.semaphore_signal(barrier, inc=1, device_id=(me, across), device_id_type=MESH)

    def load(index):
        channel, shift = index // freq_count, index % freq_count
        owner = bit_flip(me, shift, freq_count)
        return pltpu.make_async_copy(
            volts.at[owner * owned + channel],
            raw.at[index % raw_slots],
            raw_sem.at[index % raw_slots],
        )

    for index in range(raw_slots):
        load(index).start()

    @pl.when(inner)
    def _():
        pl.semaphore_wait(barrier, freq_count + 1)

    @pl.when(jnp.logical_not(inner))
    def _():
        pl.semaphore_wait(barrier, freq_count)

    def turn(channel, owner):
        return pltpu.make_async_remote_copy(
            src_ref=sent.at[channel, owner],
            dst_ref=held.at[0, channel, pl.ds(me * local_feeds, local_feeds)],
            send_sem=turn_send.at[channel, owner],
            recv_sem=turn_recv.at[channel, me],
            device_id=(owner, plane),
            device_id_type=MESH,
        )

    def turned(channel, source):
        return pltpu.make_async_remote_copy(
            src_ref=sent.at[channel, source],
            dst_ref=held.at[0, channel, pl.ds(source * local_feeds, local_feeds)],
            send_sem=turn_send.at[channel, source],
            recv_sem=turn_recv.at[channel, source],
            device_id=(source, plane),
            device_id_type=MESH,
        )

    def equalize(index, put):
        channel, shift = index // freq_count, index % freq_count
        owner = bit_flip(me, shift, freq_count)
        slot = index % raw_slots
        load(index).wait()
        which = owner * owned + channel
        tile = 16
        for start in range(0, local_feeds, tile):
            gain_real = scale[0, which, pl.ds(start, tile), :]
            gain_imag = scale[1, which, pl.ds(start, tile), :]
            for lane in range(0, samples, 128):
                real = raw[slot, pl.ds(start, tile), 0, pl.ds(lane, 128)].astype(jnp.float32)
                imag = raw[slot, pl.ds(start, tile), 1, pl.ds(lane, 128)].astype(jnp.float32)
                put(
                    channel,
                    owner,
                    start,
                    tile,
                    lane,
                    (gain_real * real - gain_imag * imag).astype(jnp.bfloat16),
                    (gain_real * imag + gain_imag * real).astype(jnp.bfloat16),
                )

        @pl.when(index + raw_slots < blocks)
        def _():
            load(index + raw_slots).start()

    def put_own(channel, owner, start, tile, lane, real, imag):
        where = pl.ds(me * local_feeds + start, tile)
        held[0, channel, where, pl.ds(lane, 128)] = real
        held[0, channel, where, pl.ds(samples + lane, 128)] = imag

    def put_sent(channel, owner, start, tile, lane, real, imag):
        sent[channel, owner, pl.ds(start, tile), pl.ds(lane, 128)] = real
        sent[channel, owner, pl.ds(start, tile), pl.ds(samples + lane, 128)] = imag

    def equalize_channel(channel):
        equalize(channel * freq_count, put_own)

        @pl.loop(1, freq_count)
        def _(shift):
            equalize(channel * freq_count + shift, put_sent)
            turn(channel, bit_flip(me, shift, freq_count)).start()

    def rows_of(step):
        return pl.ds(pl.multiple_of(bit_flip(my_pair, step, pairs) * chunk, chunk), chunk)

    def sample_copy(channel, step, source, target, send, recv, device):
        where = rows_of(step)
        return pltpu.make_async_remote_copy(
            src_ref=held.at[source, channel, where],
            dst_ref=held.at[target, channel, where],
            send_sem=send,
            recv_sem=recv,
            device_id=(me, device),
            device_id_type=MESH,
        )

    def outward(channel, step):
        return sample_copy(
            channel, step, 0, 1, out_send.at[channel, step], out_recv.at[channel, step], beside
        )

    def middle(which, channel, step):
        return sample_copy(
            channel,
            step,
            which,
            2 + which,
            mid_send.at[which, channel, step],
            mid_recv.at[which, channel, step],
            across,
        )

    def await_turn(channel, step):
        pair = bit_flip(my_pair, step, pairs)
        for core in range(2):
            source = pair * 2 + core

            @pl.when(source != me)
            def _():
                turned(channel, source).wait_recv()

    def pass_on(channel, step):
        await_turn(channel, step)

        @pl.when(inner)
        def _():
            middle(0, channel, step).start()

        @pl.when(jnp.logical_not(inner))
        def _():
            outward(channel, step).start()

    def product(left, right):
        contract = (((1,), (1,)), ((), ()))
        dot = functools.partial(
            lax.dot_general, dimension_numbers=contract, preferred_element_type=jnp.float32
        )
        real = dot(left, right)
        imag = dot(left[:, samples:], right[:, :samples]) - dot(left[:, :samples], right[:, samples:])
        return real * (1.0 / samples), imag * (1.0 / samples)

    equalize_channel(0)
    pass_on(0, 0)

    @pl.loop(1, owned)
    def _(channel):
        equalize_channel(channel)

    @pl.loop(1, pairs)
    def _(step):
        pass_on(0, step)

    def wide_copy(slot, channel, block):
        return pltpu.make_async_copy(
            wide.at[slot],
            out.at[channel, :, :, pl.ds(pl.multiple_of(block * rows, rows), rows)],
            wide_sem.at[slot],
        )

    def own_block(channel, source, block, count):
        slot = count % 2

        @pl.when(count >= 2)
        def _():
            wide_copy(slot, channel, block).wait()

        size = min(256, rows)

        @pl.loop(0, rows // size)
        def _(i):
            @pl.loop(0, rows // size)
            def _(j):
                real, imag = product(
                    held[0, channel, pl.ds(i * size, size), :],
                    held[source, channel, pl.ds(j * size, size), :],
                )
                wide[slot, 0, pl.ds(i * size, size), pl.ds(pl.multiple_of(j * size, size), size)] = real
                wide[slot, 1, pl.ds(i * size, size), pl.ds(pl.multiple_of(j * size, size), size)] = imag

        wide_copy(slot, channel, block).start()

    def vis_copy(item, slot, channel, kind, step, across_columns):
        where = rows_of(step)
        if across_columns:
            source = staged.at[slot, :, :, where]
            target = landed.at[channel, kind, :, :, where]
        else:
            source = staged.at[slot, :, where, :]
            target = landed.at[channel, kind, :, where, :]
        return pltpu.make_async_remote_copy(
            src_ref=source,
            dst_ref=target,
            send_sem=vis_send.at[slot, step],
            recv_sem=vis_recv.at[channel, kind, step],
            device_id=(me, beside),
            device_id_type=MESH,
        )

    def claim(item):
        @pl.when(item >= stage_slots)
        def _():
            for step in range(pairs):
                vis_copy(item, item % stage_slots, 0, 0, step, False).wait_send()

    def vis_rows(channel, kind, source, step):
        item = channel * 3 + kind
        slot = item % stage_slots
        where = rows_of(step)
        size = min(256, rows)

        @pl.loop(0, rows // size)
        def _(j):
            columns = pl.ds(pl.multiple_of(j * size, size), size)
            real, imag = product(held[1, channel, where, :], held[source, channel, columns, :])
            staged[slot, 0, where, columns] = real.astype(jnp.bfloat16)
            staged[slot, 1, where, columns] = imag.astype(jnp.bfloat16)

        vis_copy(item, slot, channel, kind, step, False).start()

    def vis_columns(channel, kind, source, step):
        item = channel * 3 + kind
        slot = item % stage_slots
        where = rows_of(step)
        size = min(256, rows)

        @pl.loop(0, rows // size)
        def _(i):
            lines = pl.ds(pl.multiple_of(i * size, size), size)
            real, imag = product(held[1, channel, lines, :], held[source, channel, where, :])
            staged[slot, 0, lines, where] = real.astype(jnp.bfloat16)
            staged[slot, 1, lines, where] = imag.astype(jnp.bfloat16)

        vis_copy(item, slot, channel, kind, step, True).start()

    @pl.when(inner)
    def _():
        @pl.loop(0, owned)
        def _(channel):
            claim(channel * 3)

            @pl.loop(0, pairs)
            def _(step):
                outward(channel, step).wait_recv()
                middle(1, channel, step).start()
                vis_rows(channel, 0, 0, step)

            @pl.when(channel + 1 < owned)
            def _():
                @pl.loop(0, pairs)
                def _(step):
                    await_turn(channel + 1, step)
                    middle(0, channel + 1, step).start()

            own_block(channel, 0, plane, channel * 4)
            own_block(channel, 1, beside, channel * 4 + 1)

            for step in range(pairs):
                middle(0, channel, step).wait_recv()
            claim(channel * 3 + 1)

            @pl.loop(0, pairs)
            def _(step):
                vis_rows(channel, 1, 2, step)

            own_block(channel, 2, across, channel * 4 + 2)
            claim(channel * 3 + 2)

            @pl.loop(0, pairs)
            def _(step):
                middle(1, channel, step).wait_recv()
                vis_columns(channel, 2, 3, step)

            own_block(channel, 3, 3 - beside, channel * 4 + 3)

        for back in range(2):
            wide_copy(back, 0, 0).wait()

        @pl.loop(0, owned)
        def _(channel):
            for which in range(2):
                for step in range(pairs):
                    middle(which, channel, step).wait_send()

        for slot in range(stage_slots):
            for step in range(pairs):
                vis_copy(0, slot, 0, 0, step, False).wait_send()

    @pl.when(jnp.logical_not(inner))
    def _():
        @pl.loop(1, owned)
        def _(channel):
            @pl.loop(0, pairs)
            def _(step):
                await_turn(channel, step)
                outward(channel, step).start()

        @pl.loop(0, owned)
        def _(channel):
            own_block(channel, 0, plane, channel)

        def widen(channel, kind, block, count):
            slot = count % 2
            wide_copy(slot, channel, block).wait()
            across_columns = kind == 2

            @pl.loop(0, pairs)
            def _(step):
                vis_copy(0, 0, channel, kind, step, across_columns).wait_recv()
                where = rows_of(step)
                for part in range(2):
                    if across_columns:
                        wide[slot, part, :, where] = landed[channel, kind, part, :, where].astype(jnp.float32)
                    else:
                        wide[slot, part, where, :] = landed[channel, kind, part, where, :].astype(jnp.float32)

            wide_copy(slot, channel, block).start()

        @pl.loop(0, owned)
        def _(channel):
            widen(channel, 0, beside, owned + channel * 3)
            widen(channel, 1, 3 - beside, owned + channel * 3 + 1)
            widen(channel, 2, across, owned + channel * 3 + 2)

        for back in range(2):
            wide_copy(back, 0, 0).wait()

        @pl.loop(0, owned)
        def _(channel):
            for step in range(pairs):
                outward(channel, step).wait_send()

    @pl.loop(0, owned)
    def _(channel):
        @pl.loop(1, freq_count)
        def _(shift):
            turn(channel, bit_flip(me, shift, freq_count)).wait_send()


def line_program(voltages, gains):
    channels, local_feeds, _, samples = voltages.shape
    freq_count = lax.axis_size("freq")
    feed_count = lax.axis_size("feed")
    owned = channels // freq_count
    rows = local_feeds * freq_count
    pairs = freq_count // 2
    stage_slots = 3
    raw_slots = 4
    scale = jnp.broadcast_to(gains[..., None], gains.shape + (128,))
    dma = pltpu.SemaphoreType.DMA
    return pl.pallas_call(
        functools.partial(line_kernel, (owned, freq_count, local_feeds, samples)),
        name="line",
        out_shape=jax.ShapeDtypeStruct((owned, 2, rows, rows * feed_count), jnp.float32),
        in_specs=[ANY, VMEM],
        out_specs=ANY,
        scratch_shapes=[
            pltpu.VMEM((4, owned, rows, 2 * samples), jnp.bfloat16),
            pltpu.VMEM((stage_slots, 2, rows, rows), jnp.bfloat16),
            pltpu.VMEM((owned, 3, 2, rows, rows), jnp.bfloat16),
            pltpu.VMEM((2, 2, rows, rows), jnp.float32),
            pltpu.VMEM((raw_slots, local_feeds, 2, samples), jnp.int32),
            pltpu.VMEM((owned, freq_count, local_feeds, 2 * samples), jnp.bfloat16),
            dma((raw_slots,)),
            dma((owned, freq_count)),
            dma((owned, freq_count)),
            dma((owned, pairs)),
            dma((owned, pairs)),
            dma((2, owned, pairs)),
            dma((2, owned, pairs)),
            dma((stage_slots, pairs)),
            dma((owned, 3, pairs)),
            dma((2,)),
        ],
        compiler_params=pltpu.CompilerParams(
            collective_id=0, has_side_effects=True, vmem_limit_bytes=67043328
        ),
    )(voltages, scale)


def solution(mesh):
    in_specs = (P(None, ("feed", "freq"), None, None), P(None, None, ("feed", "freq")))
    out_specs = P("freq", None, "feed", None)
    freq_count = mesh.shape["freq"]
    on_a_line = mesh.shape["feed"] == 4 and freq_count > 1 and freq_count & (freq_count - 1) == 0
    body = line_program if on_a_line else ring_program
    return jax.shard_map(body, mesh=mesh, in_specs=in_specs, out_specs=out_specs, check_vma=False)
```

```python
import functools

import jax
import jax.numpy as jnp
from jax import lax
from jax.experimental import pallas as pl
from jax.experimental.pallas import tpu as pltpu
from jax.sharding import PartitionSpec as P

MESH = pl.DeviceIdType.MESH
ANY = pl.BlockSpec(memory_space=pl.ANY)
VMEM = pl.BlockSpec(memory_space=pltpu.VMEM)


def stack_rows(own_rows, samples):
    real_part = own_rows[..., :samples]
    imag_part = own_rows[..., samples:]
    swapped = jnp.concatenate([imag_part, -real_part], axis=-1)
    return jnp.stack([own_rows, swapped], axis=0)


def correlate(stacked, columns, samples):
    product = jnp.einsum("qrk,fk->qrf", stacked, columns, preferred_element_type=jnp.float32)
    return product * (1.0 / samples)


def ring_blocks(own, count):
    forward = [(source, (source + 1) % count) for source in range(count)]
    backward = [(source, (source - 1) % count) for source in range(count)]
    half = own.shape[0] // 2
    pieces = [(0, 0, own)]
    from_left = from_right = own
    for step in range(1, count):
        if 2 * step > count:
            break
        if 2 * step == count:
            pieces.append((-step, 0, lax.ppermute(from_left[:half], "feed", forward)))
            pieces.append((-step, half, lax.ppermute(from_right[half:], "feed", backward)))
        else:
            from_left = lax.ppermute(from_left, "feed", forward)
            from_right = lax.ppermute(from_right, "feed", backward)
            pieces.append((-step, 0, from_left))
            pieces.append((step, 0, from_right))
    return pieces


def ring_program(voltages, gains):
    channels, local_feeds, _, samples = voltages.shape
    freq_count = lax.axis_size("freq")
    feed_count = lax.axis_size("feed")
    position = lax.axis_index("feed")
    owned = channels // freq_count
    rows = local_feeds * freq_count
    volts = voltages.reshape(freq_count, owned, local_feeds, 2, samples)
    scale = gains.reshape(2, freq_count, owned, local_feeds)[..., None]
    visibilities = jnp.zeros((owned, 2, rows, rows * feed_count), jnp.float32)
    for channel in range(owned):
        volt_real = volts[:, channel, :, 0].astype(jnp.float32)
        volt_imag = volts[:, channel, :, 1].astype(jnp.float32)
        gain_real = scale[0, :, channel]
        gain_imag = scale[1, :, channel]
        eq_real = gain_real * volt_real - gain_imag * volt_imag
        eq_imag = gain_real * volt_imag + gain_imag * volt_real
        blocks = jnp.concatenate([eq_real, eq_imag], axis=-1).astype(jnp.bfloat16)
        arrived = lax.all_to_all(blocks, "freq", split_axis=0, concat_axis=0, tiled=True)
        own_rows = arrived.reshape(rows, 2 * samples)
        stacked = stack_rows(own_rows, samples)
        for offset, start, block in ring_blocks(own_rows, feed_count):
            owner = lax.rem(position + offset + feed_count, feed_count)
            visibilities = lax.dynamic_update_slice(
                visibilities,
                correlate(stacked, block, samples)[None],
                (channel, 0, 0, owner * rows + start),
            )
    return visibilities


def bit_flip(index, mask, count):
    total, bit = 0, 1
    while bit < count:
        total = total + ((index // bit + mask // bit) % 2) * bit
        bit *= 2
    return total


def line_kernel(
    geometry,
    volts,
    gains,
    landed,
    full,
    held,
    staged,
    wide,
    raw,
    sent,
    scale,
    raw_sem,
    turn_send,
    turn_recv,
    out_send,
    out_recv,
    mid_send,
    mid_recv,
    in_send,
    in_recv,
    vis_send,
    vis_recv,
    wide_sem,
):
    owned, freq_count, local_feeds, samples = geometry
    rows = freq_count * local_feeds
    pairs = freq_count // 2
    chunk = 2 * local_feeds
    raw_slots = raw.shape[0]
    blocks = owned * freq_count
    channels = blocks
    early = min(2, owned - 1)

    me = lax.axis_index("freq")
    plane = lax.axis_index("feed")
    my_pair = me // 2
    inner = (plane == 1) | (plane == 2)
    across = 3 - plane
    beside = jnp.where(plane < 2, 1 - plane, 5 - plane)

    barrier = pltpu.get_barrier_semaphore()
    for shift in range(1, freq_count):
        pl.semaphore_signal(
            barrier,
            inc=1,
            device_id=(bit_flip(me, shift, freq_count), plane),
            device_id_type=MESH,
        )
    pl.semaphore_signal(barrier, inc=1, device_id=(me, beside), device_id_type=MESH)

    @pl.when(inner)
    def _():
        pl.semaphore_signal(barrier, inc=1, device_id=(me, across), device_id_type=MESH)

    def load(index):
        channel, shift = index // freq_count, index % freq_count
        owner = bit_flip(me, shift, freq_count)
        return pltpu.make_async_copy(
            volts.at[owner * owned + channel],
            raw.at[index % raw_slots],
            raw_sem.at[index % raw_slots],
        )

    for index in range(raw_slots):
        load(index).start()

    columns = jnp.transpose(gains[...])
    for which in range(scale.shape[0]):
        scale[which] = jnp.broadcast_to(columns[:local_feeds, which : which + 1], (local_feeds, 128))

    @pl.when(inner)
    def _():
        pl.semaphore_wait(barrier, freq_count + 1)

    @pl.when(jnp.logical_not(inner))
    def _():
        pl.semaphore_wait(barrier, freq_count)

    def turn(channel, owner):
        return pltpu.make_async_remote_copy(
            src_ref=sent.at[channel, owner],
            dst_ref=held.at[0, channel, pl.ds(me * local_feeds, local_feeds)],
            send_sem=turn_send.at[channel, owner],
            recv_sem=turn_recv.at[channel, me],
            device_id=(owner, plane),
            device_id_type=MESH,
        )

    def turned(channel, source):
        return pltpu.make_async_remote_copy(
            src_ref=sent.at[channel, source],
            dst_ref=held.at[0, channel, pl.ds(source * local_feeds, local_feeds)],
            send_sem=turn_send.at[channel, source],
            recv_sem=turn_recv.at[channel, source],
            device_id=(source, plane),
            device_id_type=MESH,
        )

    def equalize(index, put):
        channel, shift = index // freq_count, index % freq_count
        owner = bit_flip(me, shift, freq_count)
        slot = index % raw_slots
        load(index).wait()
        which = owner * owned + channel
        tile = 16
        for start in range(0, local_feeds, tile):
            gain_real = scale[which, pl.ds(start, tile), :]
            gain_imag = scale[channels + which, pl.ds(start, tile), :]
            for lane in range(0, samples, 128):
                real = raw[slot, pl.ds(start, tile), 0, pl.ds(lane, 128)].astype(jnp.float32)
                imag = raw[slot, pl.ds(start, tile), 1, pl.ds(lane, 128)].astype(jnp.float32)
                put(
                    channel,
                    owner,
                    start,
                    tile,
                    lane,
                    (gain_real * real - gain_imag * imag).astype(jnp.bfloat16),
                    (gain_real * imag + gain_imag * real).astype(jnp.bfloat16),
                )

        @pl.when(index + raw_slots < blocks)
        def _():
            load(index + raw_slots).start()

    def put_own(channel, owner, start, tile, lane, real, imag):
        where = pl.ds(me * local_feeds + start, tile)
        held[0, channel, where, pl.ds(lane, 128)] = real
        held[0, channel, where, pl.ds(samples + lane, 128)] = imag

    def put_sent(channel, owner, start, tile, lane, real, imag):
        sent[channel, owner, pl.ds(start, tile), pl.ds(lane, 128)] = real
        sent[channel, owner, pl.ds(start, tile), pl.ds(samples + lane, 128)] = imag

    def equalize_some(channel, first, last):
        @pl.loop(first, last)
        def _(shift):
            equalize(channel * freq_count + shift, put_sent)
            turn(channel, bit_flip(me, shift, freq_count)).start()

    def equalize_channel(channel):
        equalize(channel * freq_count, put_own)
        equalize_some(channel, 1, freq_count)

    def rows_of(step):
        return pl.ds(pl.multiple_of(bit_flip(my_pair, step, pairs) * chunk, chunk), chunk)

    def sample_copy(channel, step, source, target, send, recv, device):
        where = rows_of(step)
        return pltpu.make_async_remote_copy(
            src_ref=held.at[source, channel, where],
            dst_ref=held.at[target, channel, where],
            send_sem=send,
            recv_sem=recv,
            device_id=(me, device),
            device_id_type=MESH,
        )

    def outward(channel, step):
        return sample_copy(
            channel, step, 0, 1, out_send.at[channel, step], out_recv.at[channel, step], beside
        )

    def middle(which, channel, step):
        return sample_copy(
            channel,
            step,
            which,
            2 + which,
            mid_send.at[which, channel, step],
            mid_recv.at[which, channel, step],
            across,
        )

    def inward(channel):
        return sample_copy(channel, 0, 0, 2, in_send.at[channel], in_recv.at[channel], beside)

    def is_early(channel):
        return (channel >= 1) & (channel <= early)

    def await_turn(channel, step):
        pair = bit_flip(my_pair, step, pairs)
        for core in range(2):
            source = pair * 2 + core

            @pl.when(source != me)
            def _():
                turned(channel, source).wait_recv()

    def pass_on(channel, step):
        await_turn(channel, step)

        @pl.when(inner)
        def _():
            middle(0, channel, step).start()

        @pl.when(jnp.logical_not(inner))
        def _():
            outward(channel, step).start()

    def product(left, right):
        contract = (((1,), (1,)), ((), ()))
        dot = functools.partial(
            lax.dot_general, dimension_numbers=contract, preferred_element_type=jnp.float32
        )
        real = dot(left, right)
        imag = dot(left[:, samples:], right[:, :samples]) - dot(left[:, :samples], right[:, samples:])
        return real * (1.0 / samples), imag * (1.0 / samples)

    first = max(freq_count // 2, 2)
    equalize(0, put_own)
    equalize_some(0, 1, first)
    pass_on(0, 0)
    equalize_some(0, first, freq_count)

    def equalize_early(channel):
        equalize_channel(channel)
        await_turn(channel, 0)

        @pl.when(inner)
        def _():
            inward(channel).start()

    pl.loop(1, early + 1)(equalize_early)

    @pl.loop(1, pairs // 2 + 1)
    def _(step):
        pass_on(0, step)

    pl.loop(early + 1, owned)(equalize_channel)

    @pl.loop(pairs // 2 + 1, pairs)
    def _(step):
        pass_on(0, step)

    def wide_copy(slot, channel, kind):
        return pltpu.make_async_copy(wide.at[slot], full.at[channel, kind], wide_sem.at[slot])

    def own_block(channel, source, put):
        size = min(256, rows)

        @pl.loop(0, rows // size)
        def _(i):
            @pl.loop(0, rows // size)
            def _(j):
                lines = pl.ds(pl.multiple_of(i * size, size), size)
                where = pl.ds(pl.multiple_of(j * size, size), size)
                real, imag = product(held[0, channel, lines, :], held[source, channel, where, :])
                put(0, lines, where, real)
                put(1, lines, where, imag)

    def own_full(channel, source, kind):
        @pl.when(channel >= 1)
        def _():
            wide_copy(kind, channel, kind).wait()

        def put(part, lines, where, value):
            wide[kind, part, lines, where] = value

        own_block(channel, source, put)
        wide_copy(kind, channel, kind).start()

    def own_half(channel, source, kind):
        def put(part, lines, where, value):
            landed[channel, kind, part, lines, where] = value.astype(jnp.bfloat16)

        own_block(channel, source, put)

    def vis_copy(channel, kind, step, across_columns):
        where = rows_of(step)
        if across_columns:
            source = staged.at[kind, :, :, where]
            target = landed.at[channel, kind, :, :, where]
        else:
            source = staged.at[kind, :, where, :]
            target = landed.at[channel, kind, :, where, :]
        return pltpu.make_async_remote_copy(
            src_ref=source,
            dst_ref=target,
            send_sem=vis_send.at[kind, step],
            recv_sem=vis_recv.at[channel, kind, step],
            device_id=(me, beside),
            device_id_type=MESH,
        )

    def release(channel, kind):
        for step in range(pairs):

            @pl.when(jnp.logical_not((step == 0) & (kind == 0) & is_early(channel)))
            def _():
                vis_copy(channel, kind, step, False).wait_send()

    def claim(channel, kind):
        @pl.when(channel >= 1)
        def _():
            release(channel - 1, kind)

    def vis_rows(channel, kind, source, step):
        where = rows_of(step)
        size = min(256, rows)

        @pl.loop(0, rows // size)
        def _(j):
            columns = pl.ds(pl.multiple_of(j * size, size), size)
            real, imag = product(held[1, channel, where, :], held[source, channel, columns, :])
            staged[kind, 0, where, columns] = real.astype(jnp.bfloat16)
            staged[kind, 1, where, columns] = imag.astype(jnp.bfloat16)

        vis_copy(channel, kind, step, False).start()

    def vis_columns(channel, kind, source, step):
        where = rows_of(step)
        size = min(256, rows)

        @pl.loop(0, rows // size)
        def _(i):
            lines = pl.ds(pl.multiple_of(i * size, size), size)
            real, imag = product(held[1, channel, lines, :], held[source, channel, where, :])
            staged[kind, 0, lines, where] = real.astype(jnp.bfloat16)
            staged[kind, 1, lines, where] = imag.astype(jnp.bfloat16)

        vis_copy(channel, kind, step, True).start()

    @pl.when(inner)
    def _():
        @pl.loop(0, owned)
        def _(channel):
            @pl.loop(0, pairs)
            def _(step):
                outward(channel, step).wait_recv()
                middle(1, channel, step).start()

                @pl.when(channel == 0)
                def _():
                    vis_rows(channel, 0, 0, step)

            @pl.when(channel >= 1)
            def _():
                claim(channel, 0)

                @pl.loop(jnp.where(is_early(channel), 1, 0), pairs)
                def _(step):
                    vis_columns(channel, 0, 0, step)

            @pl.when(channel + 1 < owned)
            def _():
                @pl.loop(0, pairs)
                def _(step):
                    @pl.when(jnp.logical_not((step == 0) & is_early(channel + 1)))
                    def _():
                        await_turn(channel + 1, step)

                    middle(0, channel + 1, step).start()

            for step in range(pairs):
                middle(0, channel, step).wait_recv()
            claim(channel, 1)

            @pl.loop(0, pairs)
            def _(step):
                vis_rows(channel, 1, 2, step)

            own_full(channel, 0, 0)
            own_full(channel, 1, 1)
            own_half(channel, 2, 0)
            claim(channel, 2)

            @pl.loop(0, pairs)
            def _(step):
                middle(1, channel, step).wait_recv()
                vis_columns(channel, 2, 3, step)

            own_half(channel, 3, 1)

        for kind in range(2):
            wide_copy(kind, 0, kind).wait()

        @pl.loop(0, owned)
        def _(channel):
            for which in range(2):
                for step in range(pairs):
                    middle(which, channel, step).wait_send()

        @pl.loop(1, early + 1)
        def _(channel):
            inward(channel).wait_send()

        for kind in range(3):
            release(owned - 1, kind)

    @pl.when(jnp.logical_not(inner))
    def _():
        @pl.loop(1, owned)
        def _(channel):
            @pl.loop(0, pairs)
            def _(step):
                @pl.when(jnp.logical_not((step == 0) & is_early(channel)))
                def _():
                    await_turn(channel, step)

                outward(channel, step).start()

        @pl.loop(0, owned)
        def _(channel):
            own_full(channel, 0, 0)

        @pl.loop(0, owned)
        def _(channel):
            @pl.when(channel == 0)
            def _():
                for step in range(pairs):
                    vis_copy(channel, 0, step, False).wait_recv()

            @pl.when(channel >= 1)
            def _():
                @pl.when(is_early(channel))
                def _():
                    inward(channel).wait_recv()
                    where = rows_of(0)
                    real, imag = product(held[0, channel], held[2, channel, where, :])
                    landed[channel, 0, 0, :, where] = real.astype(jnp.bfloat16)
                    landed[channel, 0, 1, :, where] = imag.astype(jnp.bfloat16)

                @pl.loop(jnp.where(is_early(channel), 1, 0), pairs)
                def _(step):
                    vis_copy(channel, 0, step, True).wait_recv()

            for kind in range(1, 3):
                for step in range(pairs):
                    vis_copy(channel, kind, step, kind == 2).wait_recv()

        wide_copy(0, 0, 0).wait()

        @pl.loop(0, owned)
        def _(channel):
            for step in range(pairs):
                outward(channel, step).wait_send()

    @pl.loop(0, owned)
    def _(channel):
        @pl.loop(1, freq_count)
        def _(shift):
            turn(channel, bit_flip(me, shift, freq_count)).wait_send()


def line_program(voltages, gains):
    channels, local_feeds, _, samples = voltages.shape
    freq_count = lax.axis_size("freq")
    feed_count = lax.axis_size("feed")
    owned = channels // freq_count
    rows = local_feeds * freq_count
    pairs = freq_count // 2
    raw_slots = 4
    dma = pltpu.SemaphoreType.DMA
    half, full = pl.pallas_call(
        functools.partial(line_kernel, (owned, freq_count, local_feeds, samples)),
        name="line",
        out_shape=[
            pltpu.VMEM((owned, 3, 2, rows, rows), jnp.bfloat16),
            jax.ShapeDtypeStruct((owned, 2, 2, rows, rows), jnp.float32),
        ],
        in_specs=[ANY, VMEM],
        out_specs=[VMEM, ANY],
        scratch_shapes=[
            pltpu.VMEM((4, owned, rows, 2 * samples), jnp.bfloat16),
            pltpu.VMEM((3, 2, rows, rows), jnp.bfloat16),
            pltpu.VMEM((2, 2, rows, rows), jnp.float32),
            pltpu.VMEM((raw_slots, local_feeds, 2, samples), jnp.int32),
            pltpu.VMEM((owned, freq_count, local_feeds, 2 * samples), jnp.bfloat16),
            pltpu.VMEM((2 * channels, local_feeds, 128), jnp.float32),
            dma((raw_slots,)),
            dma((owned, freq_count)),
            dma((owned, freq_count)),
            dma((owned, pairs)),
            dma((owned, pairs)),
            dma((2, owned, pairs)),
            dma((2, owned, pairs)),
            dma((owned,)),
            dma((owned,)),
            dma((3, pairs)),
            dma((owned, 3, pairs)),
            dma((2,)),
        ],
        compiler_params=pltpu.CompilerParams(
            collective_id=0, has_side_effects=True, vmem_limit_bytes=48 * 2**20
        ),
    )(voltages, gains.reshape(2 * channels, local_feeds))
    return lay_out(half, full, feed_count)


def lay_out_kernel(narrow, full, out, kept, wide, kept_sem, wide_sem, out_sem):
    owned, _, _, rows, _ = narrow.shape
    slots = wide.shape[0]
    plane = lax.axis_index("feed")
    inner = (plane == 1) | (plane == 2)
    beside = jnp.where(plane < 2, 1 - plane, 5 - plane)
    across, beyond = 3 - plane, 3 - beside

    def kept_load(channel, kind):
        return pltpu.make_async_copy(
            full.at[channel, kind], kept.at[channel, kind], kept_sem.at[channel, kind]
        )

    def columns(channel, block):
        return out.at[channel, :, :, pl.ds(pl.multiple_of(block * rows, rows), rows)]

    def kept_store(channel, kind, block):
        return pltpu.make_async_copy(
            kept.at[channel, kind], columns(channel, block), out_sem.at[channel, kind]
        )

    def wide_store(slot, channel, block):
        return pltpu.make_async_copy(wide.at[slot], columns(channel, block), wide_sem.at[slot])

    def run(kept_blocks, narrow_blocks):
        @pl.loop(0, owned)
        def _(channel):
            for kind in range(len(kept_blocks)):
                kept_load(channel, kind).start()

        count = len(narrow_blocks)

        @pl.loop(0, owned)
        def _(channel):
            for kind, block in enumerate(kept_blocks):
                kept_load(channel, kind).wait()
                kept_store(channel, kind, block).start()
            for kind, block in enumerate(narrow_blocks):
                item = channel * count + kind
                slot = item % slots

                @pl.when(item >= slots)
                def _():
                    wide_store(slot, channel, block).wait()

                tile = 64

                @pl.loop(0, rows // tile)
                def _(i):
                    lines = pl.ds(pl.multiple_of(i * tile, tile), tile)
                    for part in range(2):
                        wide[slot, part, lines, :] = narrow[channel, kind, part, lines, :].astype(
                            jnp.float32
                        )

                wide_store(slot, channel, block).start()

        @pl.loop(0, owned)
        def _(channel):
            for kind, block in enumerate(kept_blocks):
                kept_store(channel, kind, block).wait()

        for slot in range(min(slots, owned * count)):
            wide_store(slot, 0, narrow_blocks[0]).wait()

    @pl.when(inner)
    def _():
        run([plane, beside], [across, beyond])

    @pl.when(jnp.logical_not(inner))
    def _():
        run([plane], [beside, beyond, across])


def lay_out(half, full, feed_count):
    owned, _, _, rows, _ = half.shape
    slots = 4
    dma = pltpu.SemaphoreType.DMA
    return pl.pallas_call(
        lay_out_kernel,
        name="lay_out",
        out_shape=jax.ShapeDtypeStruct((owned, 2, rows, rows * feed_count), jnp.float32),
        in_specs=[VMEM, ANY],
        out_specs=ANY,
        scratch_shapes=[
            pltpu.VMEM(full.shape, full.dtype),
            pltpu.VMEM((slots, 2, rows, rows), jnp.float32),
            dma((owned, 2)),
            dma((slots,)),
            dma((owned, 2)),
        ],
        compiler_params=pltpu.CompilerParams(vmem_limit_bytes=40 * 2**20),
    )(half, full)


def solution(mesh):
    in_specs = (P(None, ("feed", "freq"), None, None), P(None, None, ("feed", "freq")))
    out_specs = P("freq", None, "feed", None)
    freq_count = mesh.shape["freq"]
    on_a_line = mesh.shape["feed"] == 4 and freq_count > 1 and freq_count & (freq_count - 1) == 0
    body = line_program if on_a_line else ring_program
    return jax.shard_map(body, mesh=mesh, in_specs=in_specs, out_specs=out_specs, check_vma=False)
```
